128 devices in a mesh: batch: 1, row: 16 (over z, y), col: 8 (over x, core).
Axes of the slice: x: 4, y: 4, z: 4, core: 2. Of those that a mesh axis runs over, the one named last changes fastest.
Arguments:
- l_mat: bfloat16 [1024, 1024], P(('batch', 'row'), 'col')
- b_mat: bfloat16 [1024, 65536], P(('batch', 'row'), 'col')
Outputs:
- output: bfloat16 [1024, 65536], P(('batch', 'row'), 'col')
All inputs are finite; a program needn't handle non-finite values.
Results may differ from the reference program's by a relative error of at most 0.001.
Values are sent between devices in bfloat16 or wider.
A program may use at most 1 GiB of HBM per device.

```python
import jax
import jax.numpy as jnp

N = 1024
M = 65536


def setup_inputs(seed: int = 0, part: int = 0) -> dict:
    base_key = jax.random.fold_in(jax.random.key(seed), part)
    key_l, key_b = jax.random.split(base_key)
    row_scale = 1.0 / jnp.sqrt(jnp.arange(N, dtype=jnp.float32) + 1.0)
    l_full = jax.random.normal(key_l, (N, N), jnp.float32)
    l_mat = jnp.tril(l_full) * row_scale[:, None]
    b_mat = jax.random.normal(key_b, (N, M), jnp.float32)
    return {'l_mat': l_mat.astype(jnp.bfloat16), 'b_mat': b_mat.astype(jnp.bfloat16)}


def reference(l_mat, b_mat):
    product = jnp.dot(l_mat, b_mat, preferred_element_type=jnp.float32)
    return product.astype(jnp.bfloat16)
```

```python
import jax
import jax.numpy as jnp
from jax import lax
from jax.experimental import pallas as pl
from jax.experimental.pallas import tpu as pltpu
from jax.sharding import PartitionSpec as P

MESH = pl.DeviceIdType.MESH
RING = 4
PIECES = 2
PLANE = [(dz, dy) for dz in range(RING) for dy in range(RING) if (dz, dy) != (0, 0)]
ORDER = [(1, 1), (3, 3), (1, 3), (3, 1), (2, 1), (2, 3), (1, 2), (3, 2), (2, 2), (0, 1), (0, 3), (1, 0), (3, 0), (0, 2), (2, 0)]


def kernel(l_ref, b_ref, o_ref, b_own, b_all, l_all, x_all, load_sem, b_send, b_recv, x_send, x_recv, l_send, l_recv, s_send, s_recv, f_send, f_recv, out_sem):
    row, col = lax.axis_index('row'), lax.axis_index('col')
    z, y, x, core = row // RING, row % RING, col // 2, col % 2
    rows, width = b_all.shape[2], b_all.shape[3]
    chunk = PIECES * width

    def at(dz, dy):
        return lax.rem(z + dz, RING) * RING + lax.rem(y + dy, RING)

    def cols(r, h):
        return pl.ds(pl.multiple_of(r * chunk + h * width, width), width)

    loads = [pltpu.make_async_copy(b_ref, b_own, load_sem.at[0]),
             pltpu.make_async_copy(l_ref, l_all.at[col, pl.ds(pl.multiple_of(row * rows, rows), rows)], load_sem.at[1])]
    loads += [pltpu.make_async_copy(b_ref.at[:, cols(row, h)], b_all.at[h, row], load_sem.at[2 + h]) for h in range(PIECES)]
    for copy in loads:
        copy.start()

    barrier = pltpu.get_barrier_semaphore()
    for dz, dy in PLANE:
        pl.semaphore_signal(barrier, inc=1, device_id=(0, at(dz, dy), col), device_id_type=MESH)
    for dx in (1, 2, 3):
        pl.semaphore_signal(barrier, inc=1, device_id=(0, row, lax.rem(x + dx, RING) * 2 + core), device_id_type=MESH)
    pl.semaphore_signal(barrier, inc=1, device_id=(0, row, x * 2 + 1 - core), device_id_type=MESH)
    pl.semaphore_wait(barrier, len(PLANE) + 4)
    for copy in loads:
        copy.wait()

    def l_copy(i):
        dz, dy = ORDER[i]
        here = l_all.at[col, pl.ds(pl.multiple_of(row * rows, rows), rows)]
        return pltpu.make_async_remote_copy(src_ref=here, dst_ref=here, send_sem=l_send.at[i], recv_sem=l_recv.at[i],
                                            device_id=(0, at(dz, dy), col), device_id_type=MESH)

    @pl.when(z >= x)
    def _():
        for i in range(len(ORDER)):
            l_copy(i).start()

    def b_copy(h, i):
        peer = at(*ORDER[i])
        return pltpu.make_async_remote_copy(src_ref=b_own.at[:, cols(peer, h)], dst_ref=b_all.at[h, row], send_sem=b_send.at[h, i],
                                            recv_sem=b_recv.at[h, i], device_id=(0, peer, col), device_id_type=MESH)

    for h in range(PIECES):
        for i in range(len(ORDER)):
            b_copy(h, i).start()

    for i, (dz, dy) in enumerate(ORDER):
        @pl.when(lax.rem(z + RING - dz, RING) >= x)
        def _(i=i):
            l_copy(i).wait_recv()

    group = RING * rows

    def span(block, g):
        return l_all.at[block, pl.ds(g * group, group)]

    def s_copy(k, g):
        to = lax.rem(x + k + 1, RING) * 2 + core if k < 3 else x * 2 + 1 - core
        return pltpu.make_async_remote_copy(src_ref=span(col, g), dst_ref=span(col, g), send_sem=s_send.at[k, g], recv_sem=s_recv.at[k, g],
                                            device_id=(0, row, to), device_id_type=MESH)

    def f_copy(k, g):
        block = lax.rem(x + RING - k - 1, RING) * 2 + core
        return pltpu.make_async_remote_copy(src_ref=span(block, g), dst_ref=span(block, g), send_sem=f_send.at[k, g], recv_sem=f_recv.at[k, g],
                                            device_id=(0, row, x * 2 + 1 - core), device_id_type=MESH)

    for g in range(RING):
        @pl.when(g >= x)
        def _(g=g):
            for k in range(4):
                s_copy(k, g).start()
    for g in range(RING):
        for k in range(3):
            @pl.when(g >= lax.rem(x + RING - k - 1, RING))
            def _(k=k, g=g):
                s_copy(k, g).wait_recv()
                f_copy(k, g).start()
    for g in range(RING):
        @pl.when(g >= x)
        def _(g=g):
            s_copy(3, g).wait_recv()
        for k in range(3):
            @pl.when(g >= lax.rem(x + RING - k - 1, RING))
            def _(k=k, g=g):
                f_copy(k, g).wait_recv()

    def x_copy(h, i):
        peer = at(*ORDER[i])
        return pltpu.make_async_remote_copy(src_ref=x_all.at[h, peer], dst_ref=o_ref.at[:, cols(row, h)], send_sem=x_send.at[h, i],
                                            recv_sem=x_recv.at[h, i], device_id=(0, peer, col), device_id_type=MESH)

    outs = []
    for h in range(PIECES):
        for i in range(len(ORDER)):
            b_copy(h, i).wait_recv()
        for g in range(RING):
            depth = (g + 1) * group
            left = jnp.concatenate([l_all[k, g * group:(g + 1) * group, :] for k in range(2 * (g + 1))], axis=1)
            right = b_all[h, :(g + 1) * RING].reshape(depth, width)
            total = jnp.dot(left, right, preferred_element_type=jnp.float32)
            x_all[h, g * RING:(g + 1) * RING] = total.astype(jnp.bfloat16).reshape(RING, rows, width)
        for i in range(len(ORDER)):
            x_copy(h, i).start()
        out = pltpu.make_async_copy(x_all.at[h, row], o_ref.at[:, cols(row, h)], out_sem.at[h])
        out.start()
        outs.append(out)

    for i in range(len(ORDER)):
        @pl.when(z >= x)
        def _(i=i):
            l_copy(i).wait_send()
    for g in range(RING):
        @pl.when(g >= x)
        def _(g=g):
            for k in range(4):
                s_copy(k, g).wait_send()
        for k in range(3):
            @pl.when(g >= lax.rem(x + RING - k - 1, RING))
            def _(k=k, g=g):
                f_copy(k, g).wait_send()
    for h in range(PIECES):
        for i in range(len(ORDER)):
            b_copy(h, i).wait_send()
            x_copy(h, i).wait()
        outs[h].wait()


def solution(mesh):
    block_spec = P(('batch', 'row'), 'col')
    dma = pltpu.SemaphoreType.DMA

    def step(l_block, b_block):
        rows, columns = b_block.shape
        width = columns // 16 // PIECES
        n = len(ORDER)
        return pl.pallas_call(
            kernel,
            out_shape=jax.ShapeDtypeStruct(b_block.shape, b_block.dtype),
            in_specs=[pl.BlockSpec(memory_space=pl.ANY)] * 2,
            out_specs=pl.BlockSpec(memory_space=pl.ANY),
            scratch_shapes=[
                pltpu.VMEM((rows, columns), jnp.bfloat16),
                pltpu.VMEM((PIECES, 16, rows, width), jnp.bfloat16),
                pltpu.VMEM((8, 16 * rows, 128), jnp.bfloat16),
                pltpu.VMEM((PIECES, 16, rows, width), jnp.bfloat16),
                dma((2 + PIECES,)),
                dma((PIECES, n)), dma((PIECES, n)), dma((PIECES, n)), dma((PIECES, n)),
                dma((n,)), dma((n,)),
                dma((4, RING)), dma((4, RING)), dma((3, RING)), dma((3, RING)),
                dma((PIECES,)),
            ],
            compiler_params=pltpu.CompilerParams(collective_id=0, has_side_effects=True),
        )(l_block, b_block)

    return jax.shard_map(step, mesh=mesh, in_specs=(block_spec, block_spec), out_specs=block_spec, check_vma=False)
```

```python
import jax
import jax.numpy as jnp
from jax import lax
from jax.experimental import pallas as pl
from jax.experimental.pallas import tpu as pltpu
from jax.sharding import PartitionSpec as P

MESH = pl.DeviceIdType.MESH
RING = 4
PIECES = 2
SHIFTS = (1, 3, 2, 0)
UP = 1


def kernel(l_ref, b_ref, o_ref, b_own, b_all, l_all, x_all, load_sem, b_send, b_recv, x_send, x_recv, l_send, l_recv, s_send, s_recv, r_send,
           f_send, f_recv, out_sem, ack, ack_x):
    row, col = lax.axis_index('row'), lax.axis_index('col')
    z, y, x, core = row // RING, row % RING, col // 2, col % 2
    rows, width = b_all.shape[2], b_all.shape[3]
    chunk = PIECES * width
    group = RING * rows
    partner = x * 2 + 1 - core

    def cols(r, h):
        return pl.ds(pl.multiple_of(r * chunk + h * width, width), width)

    def there(g, dy):
        return g * RING + lax.rem(y + dy, RING)

    def others(g, act):
        for dy in SHIFTS:
            if dy:
                act(dy)
            else:
                pl.when(z != g)(lambda: act(0))

    here = l_all.at[col, pl.ds(pl.multiple_of(row * rows, rows), rows)]
    loads = [pltpu.make_async_copy(l_ref, here, load_sem.at[0]), pltpu.make_async_copy(b_ref, b_own, load_sem.at[1])]
    loads += [pltpu.make_async_copy(b_ref.at[:, cols(row, h)], b_all.at[h, row], load_sem.at[2 + h]) for h in range(PIECES)]
    for copy in loads:
        copy.start()

    barrier = pltpu.get_barrier_semaphore()

    def greet(sem, to_row, to_col):
        pl.semaphore_signal(sem, inc=1, device_id=(0, to_row, to_col), device_id_type=MESH)

    greet(barrier, row, partner)
    for dy in (1, 2, 3):
        greet(barrier, there(z, dy), col)
    for k in range(1, RING):
        @pl.when(k > x)
        def _(k=k):
            greet(barrier, row, k * 2 + core)
    for g in range(1, RING):
        @pl.when(g > z)
        def _(g=g):
            for dy in range(RING):
                greet(barrier, there(g, dy), col)
    pl.semaphore_wait(barrier, RING + RING * z + x)
    for g in range(RING - 1):
        @pl.when(g < z)
        def _(g=g):
            for dy in range(RING):
                greet(ack.at[z], there(g, dy), col)
    for k in range(RING - 1):
        @pl.when(k < x)
        def _(k=k):
            greet(ack_x.at[x], row, k * 2 + core)
    for copy in loads:
        copy.wait()

    def l_copy(g, dy):
        return pltpu.make_async_remote_copy(src_ref=here, dst_ref=here, send_sem=l_send.at[g, dy], recv_sem=l_recv.at[z, dy],
                                            device_id=(0, there(g, dy), col), device_id_type=MESH)

    def l_from(g, dy):
        return pltpu.make_async_remote_copy(src_ref=here, dst_ref=here, send_sem=l_send.at[g, dy], recv_sem=l_recv.at[g, dy],
                                            device_id=(0, there(g, dy), col), device_id_type=MESH)

    def b_copy(h, g, dy, sender):
        return pltpu.make_async_remote_copy(src_ref=b_own.at[:, cols(there(g, dy), h)], dst_ref=b_all.at[h, row], send_sem=b_send.at[h, g, dy],
                                            recv_sem=b_recv.at[h, sender, dy], device_id=(0, there(g, dy), col), device_id_type=MESH)

    for g in range(RING):
        @pl.when((g <= z) & (z >= x))
        def _(g=g):
            others(g, lambda dy: l_copy(g, dy).start())
    for g in range(RING):
        @pl.when(g > z)
        def _(g=g):
            pl.semaphore_wait(ack.at[g], RING)

            @pl.when(z >= x)
            def _():
                others(g, lambda dy: l_copy(g, dy).start())
    for h in range(PIECES):
        for g in range(RING):
            others(g, lambda dy, g=g, h=h: b_copy(h, g, dy, z).start())

    def span(block, g):
        return l_all.at[block, pl.ds(g * group, group)]

    def source(k):
        return lax.rem(x + RING - k - 1, RING)

    def s_copy(k, g):
        to = lax.rem(x + k + 1, RING) * 2 + core if k < 3 else partner
        return pltpu.make_async_remote_copy(src_ref=span(col, g), dst_ref=span(col, g), send_sem=s_send.at[k, g], recv_sem=s_recv.at[k, g],
                                            device_id=(0, row, to), device_id_type=MESH)

    def r_copy(k, g):
        part = span(source(k) * 2 + core, g)
        to = lax.rem(x + (1 if k == 0 else 3), RING) * 2 + core
        return pltpu.make_async_remote_copy(src_ref=part, dst_ref=part, send_sem=r_send.at[k, g], recv_sem=s_recv.at[1, g],
                                            device_id=(0, row, to), device_id_type=MESH)

    def f_copy(k, g):
        part = span(source(k) * 2 + core, g)
        return pltpu.make_async_remote_copy(src_ref=part, dst_ref=part, send_sem=f_send.at[k, g], recv_sem=f_recv.at[k, g],
                                            device_id=(0, row, partner), device_id_type=MESH)

    def relays(k, g):
        upward = (source(k) == 1) | (source(k) == 2) | ((source(k) == 0) & (g == UP))
        return (g >= source(k)) & (upward if k == 0 else jnp.logical_not(upward))

    for k in range(1, RING):
        @pl.when(k > x)
        def _(k=k):
            pl.semaphore_wait(ack_x.at[k], 1)
    for g in range(RING):
        @pl.when(g >= x)
        def _(g=g):
            others(g, lambda dy: l_from(g, dy).wait_recv())
            for k in (0, 2, 3):
                s_copy(k, g).start()

    def near(g):
        for k in (0, 2):
            @pl.when(g >= source(k))
            def _(k=k):
                s_copy(k, g).wait_recv()

                @pl.when(relays(k, g))
                def _():
                    r_copy(k, g).start()
                f_copy(k, g).start()

    def far(g):
        @pl.when(g >= source(1))
        def _():
            s_copy(1, g).wait_recv()
            f_copy(1, g).start()

    def across(g):
        @pl.when(g >= x)
        def _():
            s_copy(3, g).wait_recv()
        for k in range(3):
            @pl.when(g >= source(k))
            def _(k=k):
                f_copy(k, g).wait_recv()

    def x_copy(h, g, dy, sender):
        return pltpu.make_async_remote_copy(src_ref=x_all.at[h, there(g, dy)], dst_ref=o_ref.at[:, cols(row, h)], send_sem=x_send.at[h, g, dy],
                                            recv_sem=x_recv.at[h, sender, dy], device_id=(0, there(g, dy), col), device_id_type=MESH)

    def out_copy(h):
        return pltpu.make_async_copy(x_all.at[h, row], o_ref.at[:, cols(row, h)], out_sem.at[h])

    def finish(h, g):
        others(g, lambda dy: b_copy(h, g, dy, g).wait_recv())
        depth = (g + 1) * group
        left = jnp.concatenate([l_all[k, g * group:(g + 1) * group, :] for k in range(2 * (g + 1))], axis=1)
        right = b_all[h, :(g + 1) * RING].reshape(depth, width)
        total = jnp.dot(left, right, preferred_element_type=jnp.float32)
        x_all[h, g * RING:(g + 1) * RING] = total.astype(jnp.bfloat16).reshape(RING, rows, width)
        others(g, lambda dy: x_copy(h, g, dy, z).start())
        pl.when(z == g)(lambda: out_copy(h).start())

    for g in range(RING):
        near(g)
    far(0)
    for g in range(RING):
        if g + 1 < RING:
            far(g + 1)
        across(g)
        finish(0, g)
    for h in range(1, PIECES):
        for g in range(RING):
            finish(h, g)

    for g in range(RING):
        @pl.when(z >= x)
        def _(g=g):
            others(g, lambda dy: l_copy(g, dy).wait_send())

        @pl.when(g >= x)
        def _(g=g):
            for k in (0, 2, 3):
                s_copy(k, g).wait_send()
        for k in range(3):
            @pl.when(g >= source(k))
            def _(k=k, g=g):
                f_copy(k, g).wait_send()
        for k in (0, 2):
            @pl.when(relays(k, g))
            def _(k=k, g=g):
                r_copy(k, g).wait_send()
    for h in range(PIECES):
        for g in range(RING):
            others(g, lambda dy, g=g, h=h: b_copy(h, g, dy, z).wait_send())
            others(g, lambda dy, g=g, h=h: x_copy(h, g, dy, z).wait_send())
    for h in range(PIECES):
        for g in range(RING):
            others(g, lambda dy, g=g, h=h: x_copy(h, g, dy, g).wait_recv())
        out_copy(h).wait()


def solution(mesh):
    block_spec = P(('batch', 'row'), 'col')
    dma, vmem = pltpu.SemaphoreType.DMA, pltpu.VMEM

    def step(l_block, b_block):
        rows, columns = b_block.shape
        width = columns // 16 // PIECES
        pair = [dma((PIECES, RING, RING))] * 2
        return pl.pallas_call(
            kernel,
            out_shape=jax.ShapeDtypeStruct(b_block.shape, b_block.dtype),
            in_specs=[pl.BlockSpec(memory_space=pl.ANY)] * 2,
            out_specs=pl.BlockSpec(memory_space=pl.ANY),
            scratch_shapes=[
                vmem((rows, columns), jnp.bfloat16),
                vmem((PIECES, 16, rows, width), jnp.bfloat16),
                vmem((8, 16 * rows, 128), jnp.bfloat16),
                vmem((PIECES, 16, rows, width), jnp.bfloat16),
                dma((2 + PIECES,)), *pair, *pair,
                dma((RING, RING)), dma((RING, RING)),
                dma((4, RING)), dma((4, RING)), dma((3, RING)), dma((3, RING)), dma((3, RING)),
                dma((PIECES,)), pltpu.SemaphoreType.REGULAR((RING,)), pltpu.SemaphoreType.REGULAR((RING,)),
            ],
            compiler_params=pltpu.CompilerParams(collective_id=0, has_side_effects=True),
        )(l_block, b_block)

    return jax.shard_map(step, mesh=mesh, in_specs=(block_spec, block_spec), out_specs=block_spec, check_vma=False)
```

```python
import jax
import jax.numpy as jnp
from jax import lax
from jax.experimental import pallas as pl
from jax.experimental.pallas import tpu as pltpu
from jax.sharding import PartitionSpec as P

MESH = pl.DeviceIdType.MESH
RING = 4
PIECES = 2
LINES = (0, 1, 2, 3)
SHIFTS = (1, 3, 2, 0)
UP = 1


def kernel(l_ref, b_ref, o_ref, b_own, b_all, l_all, x_all, load_sem, b_send, b_recv, x_send, x_recv, l_send, l_recv, s_send, s_recv, c_send,
           c_recv, ack, ack_x, ack_core):
    row, col = lax.axis_index('row'), lax.axis_index('col')
    z, y, x, core = row // RING, row % RING, col // 2, col % 2
    rows, width = b_all.shape[2], b_all.shape[3]
    chunk = PIECES * width
    group = RING * rows
    partner = x * 2 + 1 - core

    def cols(r, h):
        return pl.ds(pl.multiple_of(r * chunk + h * width, width), width)

    def there(g, dy):
        return g * RING + lax.rem(y + dy, RING)

    def others(g, act):
        for dy in SHIFTS:
            if dy:
                act(dy)
            else:
                pl.when(z != g)(lambda: act(0))

    def line(k, act):
        for dy in SHIFTS:
            if k or dy:
                act(dy)

    here = l_all.at[col, pl.ds(pl.multiple_of(row * rows, rows), rows)]
    loads = [pltpu.make_async_copy(l_ref, here, load_sem.at[0]), pltpu.make_async_copy(b_ref, b_own, load_sem.at[1])]
    for copy in loads:
        copy.start()
    for h in range(PIECES):
        pltpu.make_async_copy(b_ref.at[:, cols(row, h)], b_all.at[h, row], load_sem.at[2]).start()
    loads.append(pltpu.make_async_copy(b_all.at[:, row], b_all.at[:, row], load_sem.at[2]))

    barrier = pltpu.get_barrier_semaphore()

    def greet(sem, to_row, to_col):
        pl.semaphore_signal(sem, inc=1, device_id=(0, to_row, to_col), device_id_type=MESH)

    pl.when(core == 1)(lambda: greet(barrier, row, partner))
    for r in range(1, RING * RING):
        pl.when(r > row)(lambda r=r: greet(barrier, r, col))
    for k in range(1, RING):
        pl.when(k > x)(lambda k=k: greet(barrier, row, k * 2 + core))
    pl.when(row + x + 1 - core > 0)(lambda: pl.semaphore_wait(barrier, row + x + 1 - core))
    for r in range(RING * RING - 1):
        pl.when(r < row)(lambda r=r: greet(ack.at[z], r, col))
    for k in range(RING - 1):
        pl.when(k < x)(lambda k=k: greet(ack_x.at[x], row, k * 2 + core))
    pl.when(core == 0)(lambda: greet(ack_core, row, partner))
    for copy in loads:
        copy.wait()

    def l_copy(g, dy):
        return pltpu.make_async_remote_copy(src_ref=here, dst_ref=here, send_sem=l_send, recv_sem=l_recv.at[z],
                                            device_id=(0, there(g, dy), col), device_id_type=MESH)

    def b_copy(h, g, dy):
        return pltpu.make_async_remote_copy(src_ref=b_own.at[:, cols(there(g, dy), h)], dst_ref=b_all.at[h, row], send_sem=b_send,
                                            recv_sem=b_recv.at[h, z], device_id=(0, there(g, dy), col), device_id_type=MESH)

    def took(ref, sem):
        pltpu.make_async_copy(ref, ref, sem).wait()

    def from_line(g, whole, less, sem):
        pl.when(z != g)(lambda: took(whole, sem))
        pl.when(z == g)(lambda: took(less, sem))

    def spread(g):
        pl.when(z >= x)(lambda: others(g, lambda dy: l_copy(g, dy).start()))

    for g in range(RING):
        pl.when(g < z)(lambda g=g: spread(g))
    for g in range(RING):
        @pl.when(g == z)
        def _(g=g):
            pl.when(y < RING - 1)(lambda: pl.semaphore_wait(ack.at[g], RING - 1 - y))
            spread(g)

        @pl.when(g > z)
        def _(g=g):
            pl.semaphore_wait(ack.at[g], RING)
            spread(g)
    for h in range(PIECES):
        for k in LINES:
            g = lax.rem(z + k, RING)
            line(k, lambda dy, g=g, h=h: b_copy(h, g, dy).start())

    def part(block, g):
        return l_all.at[block, pl.ds(g * group, group)]

    def source(k):
        return lax.rem(x + RING - k - 1, RING)

    def move(block, g, send_sem, recv_sem, to):
        return pltpu.make_async_remote_copy(src_ref=part(block, g), dst_ref=part(block, g), send_sem=send_sem, recv_sem=recv_sem,
                                            device_id=(0, row, to), device_id_type=MESH)

    def s_copy(k, g):
        return move(col, g, s_send, s_recv.at[k, g], lax.rem(x + k + 1, RING) * 2 + core)

    def r_copy(k, g):
        return move(source(k) * 2 + core, g, s_send, s_recv.at[1, g], lax.rem(x + (1 if k == 0 else 3), RING) * 2 + core)

    def c_copy(block, g):
        return move(block, g, c_send, c_recv.at[g], partner)

    def relays(k, g):
        upward = (source(k) == 1) | (source(k) == 2) | ((source(k) == 0) & (g == UP))
        return (g >= source(k)) & (upward if k == 0 else jnp.logical_not(upward))

    def first(g):
        @pl.when(g >= x)
        def _():
            from_line(g, l_all.at[0, pl.ds(0, group)], l_all.at[0, pl.ds(0, group - rows)], l_recv.at[g])
            s_copy(0, g).start()
            s_copy(2, g).start()
            c_copy(col, g).start()

    def near(g):
        for k in (0, 2):
            @pl.when(g >= source(k))
            def _(k=k):
                s_copy(k, g).wait_recv()
                pl.when(relays(k, g))(lambda: r_copy(k, g).start())
                c_copy(source(k) * 2 + core, g).start()

    def far(g):
        @pl.when(g >= source(1))
        def _():
            s_copy(1, g).wait_recv()
            c_copy(source(1) * 2 + core, g).start()

    def across(g):
        took(l_all.at[pl.ds(0, g + 1), pl.ds(0, group)], c_recv.at[g])

    for k in range(1, RING):
        pl.when(k > x)(lambda k=k: pl.semaphore_wait(ack_x.at[k], 1))
    pl.when(core == 1)(lambda: pl.semaphore_wait(ack_core, 1))
    for g in range(RING):
        first(g)
    for g in range(RING):
        near(g)

    def x_copy(h, g, dy):
        return pltpu.make_async_remote_copy(src_ref=x_all.at[h, there(g, dy)], dst_ref=o_ref.at[:, cols(row, h)], send_sem=x_send,
                                            recv_sem=x_recv, device_id=(0, there(g, dy), col), device_id_type=MESH)

    def finish(h, g):
        from_line(g, b_all.at[h, pl.ds(0, RING)], b_all.at[h, pl.ds(0, RING - 1)], b_recv.at[h, g])
        depth = (g + 1) * group
        left = jnp.concatenate([l_all[k, g * group:(g + 1) * group, :] for k in range(2 * (g + 1))], axis=1)
        right = b_all[h, :(g + 1) * RING].reshape(depth, width)
        total = jnp.dot(left, right, preferred_element_type=jnp.float32)
        x_all[h, g * RING:(g + 1) * RING] = total.astype(jnp.bfloat16).reshape(RING, rows, width)
        others(g, lambda dy: x_copy(h, g, dy).start())

    far(0)
    for g in range(RING):
        if g + 1 < RING:
            far(g + 1)
        across(g)
        finish(0, g)
    for h in range(1, PIECES):
        for g in range(RING):
            finish(h, g)
    for h in range(PIECES):
        o_ref[:, cols(row, h)] = x_all[h, row]

    pl.when(z >= x)(lambda: took(l_all.at[0, pl.ds(0, 15 * rows)], l_send))
    pl.when(x % 2 == 0)(lambda: took(l_all.at[:, pl.ds(0, group)], s_send))
    pl.when(x % 2 == 1)(lambda: took(l_all.at[pl.ds(0, 7), pl.ds(0, group)], s_send))
    took(l_all.at[pl.ds(0, 5), pl.ds(0, 2 * group)], c_send)
    took(b_all.at[:, pl.ds(0, 15)], b_send)
    took(b_all.at[:, pl.ds(0, 15)], x_send)
    took(b_all.at[:, pl.ds(0, 15)], x_recv)


def solution(mesh):
    block_spec = P(('batch', 'row'), 'col')
    dma, vmem, plain = pltpu.SemaphoreType.DMA, pltpu.VMEM, pltpu.SemaphoreType.REGULAR

    def step(l_block, b_block):
        rows, columns = b_block.shape
        width = columns // 16 // PIECES
        return pl.pallas_call(
            kernel,
            out_shape=pltpu.VMEM(b_block.shape, b_block.dtype),
            in_specs=[pl.BlockSpec(memory_space=pl.ANY)] * 2,
            out_specs=pl.BlockSpec(memory_space=pltpu.VMEM),
            scratch_shapes=[
                vmem((rows, columns), jnp.bfloat16),
                vmem((PIECES, 16, rows, width), jnp.bfloat16),
                vmem((8, 16 * rows, 128), jnp.bfloat16),
                vmem((PIECES, 16, rows, width), jnp.bfloat16),
                dma((3,)), dma(()), dma((PIECES, RING)), dma(()), dma(()), dma(()), dma((RING,)),
                dma(()), dma((3, RING)), dma(()), dma((RING,)), plain((RING,)), plain((RING,)), plain(()),
            ],
            compiler_params=pltpu.CompilerParams(collective_id=0, has_side_effects=True),
        )(l_block, b_block)

    return jax.shard_map(step, mesh=mesh, in_specs=(block_spec, block_spec), out_specs=block_spec, check_vma=False)
```

```python
import jax
import jax.numpy as jnp
from jax import lax
from jax.experimental import pallas as pl
from jax.experimental.pallas import tpu as pltpu
from jax.sharding import PartitionSpec as P

MESH = pl.DeviceIdType.MESH
RING = 4
PARTS = ((0, 256), (256, 256))
SEQUENCE = (
    ('first', 0),
    ('first', 1),
    ('first', 2),
    ('near', 0),
    ('first', 3),
    ('near', 1),
    ('far', 0),
    ('near', 2),
    ('across', 0),
    ('finish', 0, 0),
    ('far', 1),
    ('near', 3),
    ('across', 1),
    ('finish', 0, 1),
    ('far', 2),
    ('across', 2),
    ('finish', 0, 2),
    ('finish', 1, 0),
    ('far', 3),
    ('across', 3),
    ('finish', 0, 3),
    ('finish', 1, 1),
    ('finish', 1, 2),
    ('finish', 1, 3),
)
B_FIRST = ((0, 0), (1, 0))
B_ORDER = ((0, 1), (0, 2), (0, 3), (1, 1), (1, 2), (1, 3))
B_SHIFTS = (1, 3, 2, 0)
X_SHIFTS = (2, 1, 3, 0)
L_SHIFTS = (1, 3, 2, 0)
ITEMS = {
    (0, 0): (0, 0),
    (1, 0): (1, 1),
    (2, 0): (0, 0),
    (3, 0): (0, 0),
    (1, 1): (1, 1),
    (2, 1): (1, 1),
    (3, 1): (1, 1),
    (2, 2): (1, 1),
    (3, 2): (1, 1),
    (3, 3): (0, 0),
}


def kernel(l_ref, b_ref, o_ref, b_own, b_all, l_all, x_all, load_sem, b_send, b_recv, x_send, x_recv, l_send, l_recv, s_send,
           s_recv, c_send, c_recv, ack, ack_x, ack_core):
    row, col = lax.axis_index('row'), lax.axis_index('col')
    z, y, x, core = row // RING, row % RING, col // 2, col % 2
    rows, chunk = b_all.shape[1], b_all.shape[2]
    group = RING * rows
    partner = x * 2 + 1 - core

    def cols(r, h):
        return pl.ds(pl.multiple_of(r * chunk + PARTS[h][0], 128), PARTS[h][1])

    def within(h):
        return pl.ds(*PARTS[h])

    def whole(r):
        return pl.ds(pl.multiple_of(r * chunk, chunk), chunk)

    def there(g, dy):
        return g * RING + lax.rem(y + dy, RING)

    def others(g, act, shifts):
        for dy in shifts:
            if dy:
                act(dy)
            else:
                pl.when(z != g)(lambda: act(0))

    def piece(block):
        return l_all.at[block, pl.ds(pl.multiple_of(row * rows, rows), rows)]

    loads = [pltpu.make_async_copy(l_ref, piece(col), load_sem.at[0]), pltpu.make_async_copy(b_ref, b_own, load_sem.at[1]),
             pltpu.make_async_copy(b_ref.at[:, whole(row)], b_all.at[row], load_sem.at[2])]
    for copy in loads:
        copy.start()

    barrier = pltpu.get_barrier_semaphore()

    def greet(sem, to_row, to_col):
        pl.semaphore_signal(sem, inc=1, device_id=(0, to_row, to_col), device_id_type=MESH)

    pl.when(core == 1)(lambda: greet(barrier, row, partner))
    for r in range(1, RING * RING):
        pl.when(r > row)(lambda r=r: greet(barrier, r, col))
    for k in range(1, RING):
        pl.when(k > x)(lambda k=k: greet(barrier, row, k * 2 + core))
    pl.when(row + x + 1 - core > 0)(lambda: pl.semaphore_wait(barrier, row + x + 1 - core))
    for r in range(RING * RING - 1):
        pl.when(r < row)(lambda r=r: greet(ack.at[z], r, col))
    for k in range(RING - 1):
        pl.when(k < x)(lambda k=k: greet(ack_x.at[x], row, k * 2 + core))
    pl.when(core == 0)(lambda: greet(ack_core, row, partner))
    loads[0].wait()

    def took(ref, sem):
        pltpu.make_async_copy(ref, ref, sem).wait()

    def from_line(g, four, three, sem):
        pl.when(z != g)(lambda: took(four, sem))
        pl.when(z == g)(lambda: took(three, sem))

    def block(item):
        return item[1] * 2 + core

    def role(item, shift):
        return lax.rem(x + RING - item[1], RING) == shift

    def to_x(k):
        return lax.rem(x + k, RING) * 2 + core

    def l_copy(item, g, dy):
        return pltpu.make_async_remote_copy(src_ref=piece(block(item)), dst_ref=piece(block(item)), send_sem=l_send, recv_sem=l_recv.at[item[0]],
                                            device_id=(0, there(g, dy), col), device_id_type=MESH)

    def spread(g):
        for item in ITEMS:
            pl.when((z == item[0]) & role(item, 0))(lambda item=item: others(g, lambda dy: l_copy(item, g, dy).start(), L_SHIFTS))

    def b_copy(h, g, dy):
        return pltpu.make_async_remote_copy(src_ref=b_own.at[:, cols(there(g, dy), h)], dst_ref=b_all.at[row, :, within(h)], send_sem=b_send,
                                            recv_sem=b_recv.at[h, z], device_id=(0, there(g, dy), col), device_id_type=MESH)

    def b_line(h, k):
        for dy in B_SHIFTS:
            if k or dy:
                b_copy(h, lax.rem(z + k, RING), dy).start()

    for g in range(RING):
        pl.when(g < z)(lambda g=g: spread(g))
    for g in range(RING):
        @pl.when(g == z)
        def _(g=g):
            pl.when(y < RING - 1)(lambda: pl.semaphore_wait(ack.at[g], RING - 1 - y))
            spread(g)
    loads[1].wait()
    for h, k in B_FIRST:
        b_line(h, k)
    for g in range(RING):
        @pl.when(g > z)
        def _(g=g):
            pl.semaphore_wait(ack.at[g], RING)
            spread(g)
    for h, k in B_ORDER:
        b_line(h, k)
    loads[2].wait()

    def s_copy(item, k):
        part = l_all.at[block(item), pl.ds(item[0] * group, group)]
        return pltpu.make_async_remote_copy(src_ref=part, dst_ref=part, send_sem=s_send, recv_sem=s_recv.at[item[0], item[1]],
                                            device_id=(0, row, to_x(k)), device_id_type=MESH)

    def c_copy(item):
        part = l_all.at[block(item), pl.ds(item[0] * group, group)]
        return pltpu.make_async_remote_copy(src_ref=part, dst_ref=part, send_sem=c_send, recv_sem=c_recv.at[item[0]],
                                            device_id=(0, row, partner), device_id_type=MESH)

    def upward(item):
        return jnp.where(core == 0, ITEMS[item][0], ITEMS[item][1]) == 1

    def first(item):
        @pl.when(role(item, 0))
        def _():
            from_line(item[0], l_all.at[0, pl.ds(0, group)], l_all.at[0, pl.ds(0, group - rows)], l_recv.at[item[0]])
            s_copy(item, 1).start()
            s_copy(item, 3).start()
            c_copy(item).start()

    def near(item):
        @pl.when(role(item, 1) | role(item, 3))
        def _():
            s_copy(item, 1).wait_recv()
            pl.when(role(item, 1) & upward(item))(lambda: s_copy(item, 1).start())
            pl.when(role(item, 3) & jnp.logical_not(upward(item)))(lambda: s_copy(item, 3).start())
            c_copy(item).start()

    def far(item):
        @pl.when(role(item, 2))
        def _():
            s_copy(item, 1).wait_recv()
            c_copy(item).start()

    def across(g):
        took(l_all.at[pl.ds(0, g + 1), pl.ds(0, group)], c_recv.at[g])

    def each(act, g):
        for item in ITEMS:
            if item[0] == g:
                act(item)

    pl.when(core == 1)(lambda: pl.semaphore_wait(ack_core, 1))
    for k in range(1, RING):
        pl.when(k > x)(lambda k=k: pl.semaphore_wait(ack_x.at[k], 1))
    def x_copy(h, g, dy):
        return pltpu.make_async_remote_copy(src_ref=x_all.at[there(g, dy), :, within(h)], dst_ref=o_ref.at[:, cols(row, h)], send_sem=x_send,
                                            recv_sem=x_recv, device_id=(0, there(g, dy), col), device_id_type=MESH)

    def finish(h, g):
        from_line(g, b_all.at[pl.ds(0, RING), :, within(h)], b_all.at[pl.ds(0, RING - 1), :, within(h)], b_recv.at[h, g])
        depth, (start, width) = (g + 1) * group, PARTS[h]
        left = jnp.concatenate([l_all[k, g * group:(g + 1) * group, :] for k in range(2 * (g + 1))], axis=1)
        right = b_all[:(g + 1) * RING, :, start:start + width].reshape(depth, width)
        total = jnp.dot(left, right, preferred_element_type=jnp.float32)
        x_all[g * RING:(g + 1) * RING, :, start:start + width] = total.astype(jnp.bfloat16).reshape(RING, rows, width)
        others(g, lambda dy: x_copy(h, g, dy).start(), X_SHIFTS)

    stages = {'first': first, 'near': near, 'far': far}
    for name, *at in SEQUENCE:
        if name == 'across':
            across(*at)
        elif name == 'finish':
            finish(*at)
        else:
            each(stages[name], *at)
    o_ref[:, whole(row)] = x_all[row]

    units = pl.ds(0, group)
    for item in ITEMS:
        pl.when((z == item[0]) & role(item, 0))(lambda: took(l_all.at[0, pl.ds(0, 15 * rows)], l_send))
    for c in (0, 1):
        for v in range(RING):
            count = sent_along_x(c, v)
            assert 1 <= count <= 8
            pl.when((core == c) & (x == v))(lambda count=count: took(l_all.at[pl.ds(0, count), units], s_send))
    took(l_all.at[pl.ds(0, 5), pl.ds(0, 2 * group)], c_send)
    took(b_all.at[pl.ds(0, 15)], b_send)
    took(b_all.at[pl.ds(0, 15)], x_send)
    took(b_all.at[pl.ds(0, 15)], x_recv)


def sent_along_x(c, v):
    count = 0
    for (_, source), up in ITEMS.items():
        count += 2 if source == v else 0
        count += 1 if (v - source) % RING == (1 if up[c] else 3) else 0
    return count


def solution(mesh):
    block_spec = P(('batch', 'row'), 'col')
    dma, vmem, plain = pltpu.SemaphoreType.DMA, pltpu.VMEM, pltpu.SemaphoreType.REGULAR

    def step(l_block, b_block):
        rows, columns = b_block.shape
        return pl.pallas_call(
            kernel,
            out_shape=pltpu.VMEM(b_block.shape, b_block.dtype),
            in_specs=[pl.BlockSpec(memory_space=pl.ANY)] * 2,
            out_specs=pl.BlockSpec(memory_space=pltpu.VMEM),
            scratch_shapes=[
                vmem((rows, columns), jnp.bfloat16),
                vmem((16, rows, columns // 16), jnp.bfloat16),
                vmem((8, 16 * rows, 128), jnp.bfloat16),
                vmem((16, rows, columns // 16), jnp.bfloat16),
                dma((3,)), dma(()), dma((len(PARTS), RING)), dma(()), dma(()), dma(()), dma((RING,)),
                dma(()), dma((RING, RING)), dma(()), dma((RING,)), plain((RING,)), plain((RING,)), plain(()),
            ],
            compiler_params=pltpu.CompilerParams(collective_id=0, has_side_effects=True),
        )(l_block, b_block)

    return jax.shard_map(step, mesh=mesh, in_specs=(block_spec, block_spec), out_specs=block_spec, check_vma=False)
```

```python
import jax
import jax.numpy as jnp
from jax import lax
from jax.experimental import pallas as pl
from jax.experimental.pallas import tpu as pltpu
from jax.sharding import PartitionSpec as P

MESH = pl.DeviceIdType.MESH
RING = 4
PARTS = ((0, 256), (256, 256))
SEQUENCE = (
    ('first', 0),
    ('first', 1),
    ('first', 2),
    ('first', 3),
    ('near', 0),
    ('near', 1),
    ('near', 2),
    ('near', 3),
    ('far', 0),
    ('across', 0),
    ('far', 1),
    ('finish', 0, 0),
    ('far', 2),
    ('across', 1),
    ('finish', 0, 1),
    ('far', 3),
    ('across', 2),
    ('finish', 0, 2),
    ('finish', 1, 0),
    ('across', 3),
    ('finish', 0, 3),
    ('finish', 1, 1),
    ('finish', 1, 2),
    ('finish', 1, 3),
)
B_FIRST = ((0, 0), (1, 0))
B_ORDER = ((0, 1), (0, 2), (0, 3), (1, 1), (1, 2), (1, 3))
B_SHIFTS = (1, 3, 2, 0)
X_SHIFTS = (1, 3, 2, 0)
L_SHIFTS = (1, 3, 2, 0)
ITEMS = {
    (0, 0): (0, 0),
    (1, 0): (1, 1),
    (2, 0): (0, 0),
    (3, 0): (0, 0),
    (1, 1): (1, 1),
    (2, 1): (1, 1),
    (3, 1): (1, 1),
    (2, 2): (1, 1),
    (3, 2): (1, 1),
    (3, 3): (0, 0),
}


def kernel(l_ref, b_ref, o_ref, b_own, b_all, l_all, x_all, load_sem, b_send, b_recv, x_send, x_recv, l_send, l_recv, s_send,
           s_recv, c_send, c_recv, ack, ack_x, ack_core):
    row, col = lax.axis_index('row'), lax.axis_index('col')
    z, y, x, core = row // RING, row % RING, col // 2, col % 2
    rows, chunk = b_all.shape[1], b_all.shape[2]
    group = RING * rows
    partner = x * 2 + 1 - core

    def cols(r, h):
        return pl.ds(pl.multiple_of(r * chunk + PARTS[h][0], 128), PARTS[h][1])

    def within(h):
        return pl.ds(*PARTS[h])

    def whole(r):
        return pl.ds(pl.multiple_of(r * chunk, chunk), chunk)

    def there(g, dy):
        return g * RING + lax.rem(y + dy, RING)

    def others(g, act, shifts):
        for dy in shifts:
            if dy:
                act(dy)
            else:
                pl.when(z != g)(lambda: act(0))

    def piece(block):
        return l_all.at[block, pl.ds(pl.multiple_of(row * rows, rows), rows)]

    loads = [pltpu.make_async_copy(l_ref, piece(col), load_sem.at[0]), pltpu.make_async_copy(b_ref, b_own, load_sem.at[1]),
             pltpu.make_async_copy(b_ref.at[:, whole(row)], b_all.at[row], load_sem.at[2])]
    for copy in loads:
        copy.start()

    barrier = pltpu.get_barrier_semaphore()

    def greet(sem, to_row, to_col):
        pl.semaphore_signal(sem, inc=1, device_id=(0, to_row, to_col), device_id_type=MESH)

    pl.when(core == 1)(lambda: greet(barrier, row, partner))
    for r in range(1, RING * RING):
        pl.when(r > row)(lambda r=r: greet(barrier, r, col))
    for k in range(1, RING):
        pl.when(k > x)(lambda k=k: greet(barrier, row, k * 2 + core))
    pl.when(row + x + 1 - core > 0)(lambda: pl.semaphore_wait(barrier, row + x + 1 - core))
    for r in range(RING * RING - 1):
        pl.when(r < row)(lambda r=r: greet(ack.at[z], r, col))
    for k in range(RING - 1):
        pl.when(k < x)(lambda k=k: greet(ack_x.at[x], row, k * 2 + core))
    pl.when(core == 0)(lambda: greet(ack_core, row, partner))
    loads[0].wait()

    def took(ref, sem):
        pltpu.make_async_copy(ref, ref, sem).wait()

    def from_line(g, four, three, sem):
        pl.when(z != g)(lambda: took(four, sem))
        pl.when(z == g)(lambda: took(three, sem))

    def block(item):
        return item[1] * 2 + core

    def role(item, shift):
        return lax.rem(x + RING - item[1], RING) == shift

    def to_x(k):
        return lax.rem(x + k, RING) * 2 + core

    def l_copy(item, g, dy):
        return pltpu.make_async_remote_copy(src_ref=piece(block(item)), dst_ref=piece(block(item)), send_sem=l_send, recv_sem=l_recv.at[item[0]],
                                            device_id=(0, there(g, dy), col), device_id_type=MESH)

    def spread(g):
        for item in ITEMS:
            pl.when((z == item[0]) & role(item, 0))(lambda item=item: others(g, lambda dy: l_copy(item, g, dy).start(), L_SHIFTS))

    def b_copy(h, g, dy):
        return pltpu.make_async_remote_copy(src_ref=b_own.at[:, cols(there(g, dy), h)], dst_ref=b_all.at[row, :, within(h)], send_sem=b_send,
                                            recv_sem=b_recv.at[h, z], device_id=(0, there(g, dy), col), device_id_type=MESH)

    def b_line(h, k):
        for dy in B_SHIFTS:
            if k or dy:
                b_copy(h, lax.rem(z + k, RING), dy).start()

    for g in range(RING):
        pl.when(g < z)(lambda g=g: spread(g))
    for g in range(RING):
        @pl.when(g == z)
        def _(g=g):
            pl.when(y < RING - 1)(lambda: pl.semaphore_wait(ack.at[g], RING - 1 - y))
            spread(g)
    loads[1].wait()
    for h, k in B_FIRST:
        b_line(h, k)
    for g in range(RING):
        @pl.when(g > z)
        def _(g=g):
            pl.semaphore_wait(ack.at[g], RING)
            spread(g)
    for h, k in B_ORDER:
        b_line(h, k)
    loads[2].wait()

    def s_copy(item, k):
        part = l_all.at[block(item), pl.ds(item[0] * group, group)]
        return pltpu.make_async_remote_copy(src_ref=part, dst_ref=part, send_sem=s_send, recv_sem=s_recv.at[list(ITEMS).index(item)],
                                            device_id=(0, row, to_x(k)), device_id_type=MESH)

    def c_copy(item):
        part = l_all.at[block(item), pl.ds(item[0] * group, group)]
        return pltpu.make_async_remote_copy(src_ref=part, dst_ref=part, send_sem=c_send, recv_sem=c_recv.at[item[0]],
                                            device_id=(0, row, partner), device_id_type=MESH)

    def upward(item):
        return jnp.where(core == 0, ITEMS[item][0], ITEMS[item][1]) == 1

    def first(item):
        @pl.when(role(item, 0))
        def _():
            from_line(item[0], l_all.at[0, pl.ds(0, group)], l_all.at[0, pl.ds(0, group - rows)], l_recv.at[item[0]])
            s_copy(item, 1).start()
            s_copy(item, 3).start()
            c_copy(item).start()

    def near(item):
        @pl.when(role(item, 1) | role(item, 3))
        def _():
            s_copy(item, 1).wait_recv()
            pl.when(role(item, 1) & upward(item))(lambda: s_copy(item, 1).start())
            pl.when(role(item, 3) & jnp.logical_not(upward(item)))(lambda: s_copy(item, 3).start())
            c_copy(item).start()

    def far(item):
        @pl.when(role(item, 2))
        def _():
            s_copy(item, 1).wait_recv()
            c_copy(item).start()

    def across(g):
        took(l_all.at[pl.ds(0, g + 1), pl.ds(0, group)], c_recv.at[g])

    def each(act, g):
        for item in ITEMS:
            if item[0] == g:
                act(item)

    pl.when(core == 1)(lambda: pl.semaphore_wait(ack_core, 1))
    for k in range(1, RING):
        pl.when(k > x)(lambda k=k: pl.semaphore_wait(ack_x.at[k], 1))
    def x_copy(h, g, dy):
        return pltpu.make_async_remote_copy(src_ref=x_all.at[there(g, dy), :, within(h)], dst_ref=o_ref.at[:, cols(row, h)], send_sem=x_send,
                                            recv_sem=x_recv, device_id=(0, there(g, dy), col), device_id_type=MESH)

    def finish(h, g):
        from_line(g, b_all.at[pl.ds(0, RING), :, within(h)], b_all.at[pl.ds(0, RING - 1), :, within(h)], b_recv.at[h, g])
        depth, (start, width) = (g + 1) * group, PARTS[h]
        left = jnp.concatenate([l_all[k, g * group:(g + 1) * group, :] for k in range(2 * (g + 1))], axis=1)
        right = b_all[:(g + 1) * RING, :, start:start + width].reshape(depth, width)
        total = jnp.dot(left, right, preferred_element_type=jnp.float32)
        x_all[g * RING:(g + 1) * RING, :, start:start + width] = total.astype(jnp.bfloat16).reshape(RING, rows, width)
        others(g, lambda dy: x_copy(h, g, dy).start(), X_SHIFTS)

    stages = {'first': first, 'near': near, 'far': far}
    for name, *at in SEQUENCE:
        if name == 'across':
            across(*at)
        elif name == 'finish':
            finish(*at)
        else:
            each(stages[name], *at)
    o_ref[:, whole(row)] = x_all[row]

    units = pl.ds(0, group)
    for item in ITEMS:
        pl.when((z == item[0]) & role(item, 0))(lambda: took(l_all.at[0, pl.ds(0, 15 * rows)], l_send))
    for c in (0, 1):
        for v in range(RING):
            count = sent_along_x(c, v)
            assert 1 <= count <= 8
            pl.when((core == c) & (x == v))(lambda count=count: took(l_all.at[pl.ds(0, count), units], s_send))
    took(l_all.at[pl.ds(0, 5), pl.ds(0, 2 * group)], c_send)
    took(b_all.at[pl.ds(0, 15)], b_send)
    took(b_all.at[pl.ds(0, 15)], x_send)
    took(b_all.at[pl.ds(0, 15)], x_recv)


def sent_along_x(c, v):
    count = 0
    for (_, source), up in ITEMS.items():
        count += 2 if source == v else 0
        count += 1 if (v - source) % RING == (1 if up[c] else 3) else 0
    return count


def solution(mesh):
    block_spec = P(('batch', 'row'), 'col')
    dma, vmem, plain = pltpu.SemaphoreType.DMA, pltpu.VMEM, pltpu.SemaphoreType.REGULAR

    def step(l_block, b_block):
        rows, columns = b_block.shape
        return pl.pallas_call(
            kernel,
            out_shape=pltpu.VMEM(b_block.shape, b_block.dtype),
            in_specs=[pl.BlockSpec(memory_space=pl.ANY)] * 2,
            out_specs=pl.BlockSpec(memory_space=pltpu.VMEM),
            scratch_shapes=[
                vmem((rows, columns), jnp.bfloat16),
                vmem((16, rows, columns // 16), jnp.bfloat16),
                vmem((8, 16 * rows, 128), jnp.bfloat16),
                vmem((16, rows, columns // 16), jnp.bfloat16),
                dma((3,)), dma(()), dma((len(PARTS), RING)), dma(()), dma(()), dma(()), dma((RING,)),
                dma(()), dma((len(ITEMS),)), dma(()), dma((RING,)), plain((RING,)), plain((RING,)), plain(()),
            ],
            compiler_params=pltpu.CompilerParams(collective_id=0, has_side_effects=True),
        )(l_block, b_block)

    return jax.shard_map(step, mesh=mesh, in_specs=(block_spec, block_spec), out_specs=block_spec, check_vma=False)
```

```python
import jax
import jax.numpy as jnp
from jax import lax
from jax.experimental import pallas as pl
from jax.experimental.pallas import tpu as pltpu
from jax.sharding import PartitionSpec as P

MESH = pl.DeviceIdType.MESH
RING = 4
PARTS = ((0, 256), (256, 256))
SEQUENCE = (
    ('first', 0),
    ('first', 1),
    ('first', 2),
    ('near', 0),
    ('first', 3),
    ('near', 1),
    ('far', 0),
    ('near', 2),
    ('across', 0),
    ('finish', 0, 0),
    ('far', 1),
    ('near', 3),
    ('across', 1),
    ('finish', 0, 1),
    ('far', 2),
    ('across', 2),
    ('finish', 0, 2),
    ('finish', 1, 0),
    ('far', 3),
    ('across', 3),
    ('finish', 0, 3),
    ('finish', 1, 1),
    ('finish', 1, 2),
    ('finish', 1, 3),
)
B_FIRST = ((0, 0), (1, 0))
B_ORDER = ((0, 1), (0, 2), (0, 3), (1, 1), (1, 2), (1, 3))
B_SHIFTS = (1, 3, 2, 0)
X_SHIFTS = (2, 1, 3, 0)
L_SHIFTS = (1, 3, 2, 0)
ITEMS = {
    (0, 0): (0, 0),
    (1, 0): (1, 1),
    (2, 0): (0, 0),
    (3, 0): (0, 0),
    (1, 1): (1, 1),
    (2, 1): (1, 1),
    (3, 1): (1, 1),
    (2, 2): (1, 1),
    (3, 2): (1, 1),
    (3, 3): (0, 0),
}


def kernel(l_ref, b_ref, o_ref, b_own, b_all, l_all, x_all, load_sem, b_send, b_recv, x_send, x_recv, l_send, l_recv, s_send,
           s_recv, c_send, c_recv, ack, ack_x, ack_core):
    row, col = lax.axis_index('row'), lax.axis_index('col')
    z, y, x, core = row // RING, row % RING, col // 2, col % 2
    rows, chunk = b_all.shape[1], b_all.shape[2]
    group = RING * rows
    partner = x * 2 + 1 - core

    def cols(r, h):
        return pl.ds(pl.multiple_of(r * chunk + PARTS[h][0], 128), PARTS[h][1])

    def within(h):
        return pl.ds(*PARTS[h])

    def whole(r):
        return pl.ds(pl.multiple_of(r * chunk, chunk), chunk)

    def there(g, dy):
        return g * RING + lax.rem(y + dy, RING)

    def others(g, act, shifts):
        for dy in shifts:
            if dy:
                act(dy)
            else:
                pl.when(z != g)(lambda: act(0))

    def piece(block):
        return l_all.at[block, pl.ds(pl.multiple_of(row * rows, rows), rows)]

    loads = [pltpu.make_async_copy(l_ref, piece(col), load_sem.at[0]), pltpu.make_async_copy(b_ref, b_own, load_sem.at[1]),
             pltpu.make_async_copy(b_ref.at[:, whole(row)], b_all.at[row], load_sem.at[2])]
    for copy in loads:
        copy.start()

    barrier = pltpu.get_barrier_semaphore()

    def greet(sem, to_row, to_col):
        pl.semaphore_signal(sem, inc=1, device_id=(0, to_row, to_col), device_id_type=MESH)

    pl.when(core == 1)(lambda: greet(barrier, row, partner))
    for r in range(1, RING * RING):
        pl.when(r > row)(lambda r=r: greet(barrier, r, col))
    for k in range(1, RING):
        pl.when(k > x)(lambda k=k: greet(barrier, row, k * 2 + core))
    pl.when(row + x + 1 - core > 0)(lambda: pl.semaphore_wait(barrier, row + x + 1 - core))
    for r in range(RING * RING - 1):
        pl.when(r < row)(lambda r=r: greet(ack.at[z], r, col))
    for k in range(RING - 1):
        pl.when(k < x)(lambda k=k: greet(ack_x.at[x], row, k * 2 + core))
    pl.when(core == 0)(lambda: greet(ack_core, row, partner))
    loads[0].wait()

    def took(ref, sem):
        pltpu.make_async_copy(ref, ref, sem).wait()

    def from_line(g, four, three, sem):
        pl.when(z != g)(lambda: took(four, sem))
        pl.when(z == g)(lambda: took(three, sem))

    def block(item):
        return item[1] * 2 + core

    def role(item, shift):
        return lax.rem(x + RING - item[1], RING) == shift

    def to_x(k):
        return lax.rem(x + k, RING) * 2 + core

    def l_copy(item, g, dy):
        return pltpu.make_async_remote_copy(src_ref=piece(block(item)), dst_ref=piece(block(item)), send_sem=l_send, recv_sem=l_recv.at[item[0]],
                                            device_id=(0, there(g, dy), col), device_id_type=MESH)

    def spread(g):
        for item in ITEMS:
            pl.when((z == item[0]) & role(item, 0))(lambda item=item: others(g, lambda dy: l_copy(item, g, dy).start(), L_SHIFTS))

    def b_copy(h, g, dy):
        return pltpu.make_async_remote_copy(src_ref=b_own.at[:, cols(there(g, dy), h)], dst_ref=b_all.at[row, :, within(h)], send_sem=b_send,
                                            recv_sem=b_recv.at[h, z], device_id=(0, there(g, dy), col), device_id_type=MESH)

    def b_line(h, k):
        for dy in B_SHIFTS:
            if k or dy:
                b_copy(h, lax.rem(z + k, RING), dy).start()

    for g in range(RING):
        pl.when(g < z)(lambda g=g: spread(g))
    for g in range(RING):
        @pl.when(g == z)
        def _(g=g):
            pl.when(y < RING - 1)(lambda: pl.semaphore_wait(ack.at[g], RING - 1 - y))
            spread(g)
    loads[1].wait()
    for h, k in B_FIRST:
        b_line(h, k)
    for g in range(RING):
        @pl.when(g > z)
        def _(g=g):
            pl.semaphore_wait(ack.at[g], RING)
            spread(g)
    for h, k in B_ORDER:
        b_line(h, k)
    loads[2].wait()

    def s_copy(item, k):
        part = l_all.at[block(item), pl.ds(item[0] * group, group)]
        return pltpu.make_async_remote_copy(src_ref=part, dst_ref=part, send_sem=s_send, recv_sem=s_recv.at[list(ITEMS).index(item)],
                                            device_id=(0, row, to_x(k)), device_id_type=MESH)

    def c_copy(item):
        part = l_all.at[block(item), pl.ds(item[0] * group, group)]
        return pltpu.make_async_remote_copy(src_ref=part, dst_ref=part, send_sem=c_send, recv_sem=c_recv.at[item[0]],
                                            device_id=(0, row, partner), device_id_type=MESH)

    def upward(item):
        return jnp.where(core == 0, ITEMS[item][0], ITEMS[item][1]) == 1

    def first(item):
        @pl.when(role(item, 0))
        def _():
            from_line(item[0], l_all.at[0, pl.ds(0, group)], l_all.at[0, pl.ds(0, group - rows)], l_recv.at[item[0]])
            s_copy(item, 1).start()
            s_copy(item, 3).start()
            c_copy(item).start()

    def near(item):
        @pl.when(role(item, 1) | role(item, 3))
        def _():
            s_copy(item, 1).wait_recv()
            pl.when(role(item, 1) & upward(item))(lambda: s_copy(item, 1).start())
            pl.when(role(item, 3) & jnp.logical_not(upward(item)))(lambda: s_copy(item, 3).start())
            c_copy(item).start()

    def far(item):
        @pl.when(role(item, 2))
        def _():
            s_copy(item, 1).wait_recv()
            c_copy(item).start()

    def across(g):
        took(l_all.at[pl.ds(0, g + 1), pl.ds(0, group)], c_recv.at[g])

    def each(act, g):
        for item in ITEMS:
            if item[0] == g:
                act(item)

    pl.when(core == 1)(lambda: pl.semaphore_wait(ack_core, 1))
    for k in range(1, RING):
        pl.when(k > x)(lambda k=k: pl.semaphore_wait(ack_x.at[k], 1))
    def x_copy(h, g, dy):
        return pltpu.make_async_remote_copy(src_ref=x_all.at[there(g, dy), :, within(h)], dst_ref=o_ref.at[:, cols(row, h)], send_sem=x_send,
                                            recv_sem=x_recv, device_id=(0, there(g, dy), col), device_id_type=MESH)

    def finish(h, g):
        from_line(g, b_all.at[pl.ds(0, RING), :, within(h)], b_all.at[pl.ds(0, RING - 1), :, within(h)], b_recv.at[h, g])
        depth, (start, width) = (g + 1) * group, PARTS[h]
        left = jnp.concatenate([l_all[k, g * group:(g + 1) * group, :] for k in range(2 * (g + 1))], axis=1)
        right = b_all[:(g + 1) * RING, :, start:start + width].reshape(depth, width)
        total = jnp.dot(left, right, preferred_element_type=jnp.float32)
        x_all[g * RING:(g + 1) * RING, :, start:start + width] = total.astype(jnp.bfloat16).reshape(RING, rows, width)
        others(g, lambda dy: x_copy(h, g, dy).start(), X_SHIFTS)

    stages = {'first': first, 'near': near, 'far': far}
    for name, *at in SEQUENCE:
        if name == 'across':
            across(*at)
        elif name == 'finish':
            finish(*at)
        else:
            each(stages[name], *at)
    o_ref[:, whole(row)] = x_all[row]

    units = pl.ds(0, group)
    for item in ITEMS:
        pl.when((z == item[0]) & role(item, 0))(lambda: took(l_all.at[0, pl.ds(0, 15 * rows)], l_send))
    for c in (0, 1):
        for v in range(RING):
            count = sent_along_x(c, v)
            assert 1 <= count <= 8
            pl.when((core == c) & (x == v))(lambda count=count: took(l_all.at[pl.ds(0, count), units], s_send))
    took(l_all.at[pl.ds(0, 5), pl.ds(0, 2 * group)], c_send)
    took(b_all.at[pl.ds(0, 15)], b_send)
    took(b_all.at[pl.ds(0, 15)], x_send)
    took(b_all.at[pl.ds(0, 15)], x_recv)


def sent_along_x(c, v):
    count = 0
    for (_, source), up in ITEMS.items():
        count += 2 if source == v else 0
        count += 1 if (v - source) % RING == (1 if up[c] else 3) else 0
    return count


def solution(mesh):
    block_spec = P(('batch', 'row'), 'col')
    dma, vmem, plain = pltpu.SemaphoreType.DMA, pltpu.VMEM, pltpu.SemaphoreType.REGULAR

    def step(l_block, b_block):
        rows, columns = b_block.shape
        return pl.pallas_call(
            kernel,
            out_shape=pltpu.VMEM(b_block.shape, b_block.dtype),
            in_specs=[pl.BlockSpec(memory_space=pl.ANY)] * 2,
            out_specs=pl.BlockSpec(memory_space=pltpu.VMEM),
            scratch_shapes=[
                vmem((rows, columns), jnp.bfloat16),
                vmem((16, rows, columns // 16), jnp.bfloat16),
                vmem((8, 16 * rows, 128), jnp.bfloat16),
                vmem((16, rows, columns // 16), jnp.bfloat16),
                dma((3,)), dma(()), dma((len(PARTS), RING)), dma(()), dma(()), dma(()), dma((RING,)),
                dma(()), dma((len(ITEMS),)), dma(()), dma((RING,)), plain((RING,)), plain((RING,)), plain(()),
            ],
            compiler_params=pltpu.CompilerParams(collective_id=0, has_side_effects=True),
        )(l_block, b_block)

    return jax.shard_map(step, mesh=mesh, in_specs=(block_spec, block_spec), out_specs=block_spec, check_vma=False)
```

```python
import jax
import jax.numpy as jnp
from jax import lax
from jax.experimental import pallas as pl
from jax.experimental.pallas import tpu as pltpu
from jax.sharding import PartitionSpec as P

MESH = pl.DeviceIdType.MESH
RING = 4
PARTS = ((0, 256), (256, 256))
SEQUENCE = (
    ('first', 0),
    ('first', 1),
    ('first', 2),
    ('near', 0),
    ('first', 3),
    ('near', 1),
    ('far', 0),
    ('near', 2),
    ('across', 0),
    ('finish', 0, 0),
    ('far', 1),
    ('near', 3),
    ('across', 1),
    ('finish', 0, 1),
    ('far', 2),
    ('across', 2),
    ('finish', 0, 2),
    ('finish', 1, 0),
    ('far', 3),
    ('across', 3),
    ('finish', 0, 3),
    ('finish', 1, 1),
    ('finish', 1, 2),
    ('finish', 1, 3),
)
B_FIRST = ((0, 0), (1, 0))
B_ORDER = ((0, 1), (0, 2), (0, 3), (1, 1), (1, 2), (1, 3))
B_SHIFTS = (1, 3, 2, 0)
X_SHIFTS = (2, 1, 3, 0)
L_SHIFTS = (1, 3, 2, 0)
ITEMS = {
    (0, 0): (0, 0),
    (1, 0): (1, 1),
    (2, 0): (0, 0),
    (3, 0): (0, 0),
    (1, 1): (1, 1),
    (2, 1): (1, 1),
    (3, 1): (1, 1),
    (2, 2): (1, 1),
    (3, 2): (1, 1),
    (3, 3): (0, 0),
}


def kernel(l_ref, b_ref, o_ref, b_own, b_all, l_all, x_all, load_sem, b_send, b_recv, x_recv, l_send, l_recv, s_send,
           s_recv, c_send, c_recv, ack, ack_x, ack_core):
    row, col = lax.axis_index('row'), lax.axis_index('col')
    z, y, x, core = row // RING, row % RING, col // 2, col % 2
    rows, chunk = b_all.shape[1], b_all.shape[2]
    group = RING * rows
    partner = x * 2 + 1 - core

    def cols(r, h):
        return pl.ds(pl.multiple_of(r * chunk + PARTS[h][0], 128), PARTS[h][1])

    def within(h):
        return pl.ds(*PARTS[h])

    def whole(r):
        return pl.ds(pl.multiple_of(r * chunk, chunk), chunk)

    def there(g, dy):
        return g * RING + lax.rem(y + dy, RING)

    def others(g, act, shifts):
        for dy in shifts:
            if dy:
                act(dy)
            else:
                pl.when(z != g)(lambda: act(0))

    def piece(block):
        return l_all.at[block, pl.ds(pl.multiple_of(row * rows, rows), rows)]

    loads = [pltpu.make_async_copy(l_ref, piece(col), load_sem.at[0]), pltpu.make_async_copy(b_ref, b_own, load_sem.at[1]),
             pltpu.make_async_copy(b_ref.at[:, whole(row)], b_all.at[row], load_sem.at[2])]
    for copy in loads:
        copy.start()

    barrier = pltpu.get_barrier_semaphore()

    def greet(sem, to_row, to_col):
        pl.semaphore_signal(sem, inc=1, device_id=(0, to_row, to_col), device_id_type=MESH)

    pl.when(core == 1)(lambda: greet(barrier, row, partner))
    for r in range(1, RING * RING):
        pl.when(r > row)(lambda r=r: greet(barrier, r, col))
    for k in range(1, RING):
        pl.when(k > x)(lambda k=k: greet(barrier, row, k * 2 + core))
    pl.when(row + x + 1 - core > 0)(lambda: pl.semaphore_wait(barrier, row + x + 1 - core))
    for r in range(RING * RING - 1):
        pl.when(r < row)(lambda r=r: greet(ack.at[z], r, col))
    for k in range(RING - 1):
        pl.when(k < x)(lambda k=k: greet(ack_x.at[x], row, k * 2 + core))
    pl.when(core == 0)(lambda: greet(ack_core, row, partner))
    loads[0].wait()

    def took(ref, sem):
        pltpu.make_async_copy(ref, ref, sem).wait()

    def from_line(g, four, three, sem):
        pl.when(z != g)(lambda: took(four, sem))
        pl.when(z == g)(lambda: took(three, sem))

    def block(item):
        return item[1] * 2 + core

    def role(item, shift):
        return lax.rem(x + RING - item[1], RING) == shift

    def to_x(k):
        return lax.rem(x + k, RING) * 2 + core

    def l_copy(item, g, dy):
        return pltpu.make_async_remote_copy(src_ref=piece(block(item)), dst_ref=piece(block(item)), send_sem=l_send, recv_sem=l_recv.at[item[0]],
                                            device_id=(0, there(g, dy), col), device_id_type=MESH)

    def spread(g):
        for item in ITEMS:
            pl.when((z == item[0]) & role(item, 0))(lambda item=item: others(g, lambda dy: l_copy(item, g, dy).start(), L_SHIFTS))

    def b_copy(h, g, dy):
        return pltpu.make_async_remote_copy(src_ref=b_own.at[:, cols(there(g, dy), h)], dst_ref=b_all.at[row, :, within(h)], send_sem=b_send,
                                            recv_sem=b_recv.at[h, z], device_id=(0, there(g, dy), col), device_id_type=MESH)

    def b_line(h, k):
        for dy in B_SHIFTS:
            if k or dy:
                b_copy(h, lax.rem(z + k, RING), dy).start()

    for g in range(RING):
        pl.when(g < z)(lambda g=g: spread(g))
    for g in range(RING):
        @pl.when(g == z)
        def _(g=g):
            pl.when(y < RING - 1)(lambda: pl.semaphore_wait(ack.at[g], RING - 1 - y))
            spread(g)
    loads[1].wait()
    for h, k in B_FIRST:
        b_line(h, k)
    for g in range(RING):
        @pl.when(g > z)
        def _(g=g):
            pl.semaphore_wait(ack.at[g], RING)
            spread(g)
    for h, k in B_ORDER:
        b_line(h, k)
    loads[2].wait()

    def s_copy(item, k):
        part = l_all.at[block(item), pl.ds(item[0] * group, group)]
        return pltpu.make_async_remote_copy(src_ref=part, dst_ref=part, send_sem=s_send, recv_sem=s_recv.at[list(ITEMS).index(item)],
                                            device_id=(0, row, to_x(k)), device_id_type=MESH)

    def c_copy(item):
        part = l_all.at[block(item), pl.ds(item[0] * group, group)]
        return pltpu.make_async_remote_copy(src_ref=part, dst_ref=part, send_sem=c_send, recv_sem=c_recv.at[item[0]],
                                            device_id=(0, row, partner), device_id_type=MESH)

    def upward(item):
        return jnp.where(core == 0, ITEMS[item][0], ITEMS[item][1]) == 1

    def first(item):
        @pl.when(role(item, 0))
        def _():
            from_line(item[0], l_all.at[0, pl.ds(0, group)], l_all.at[0, pl.ds(0, group - rows)], l_recv.at[item[0]])
            s_copy(item, 1).start()
            s_copy(item, 3).start()
            c_copy(item).start()

    def near(item):
        @pl.when(role(item, 1) | role(item, 3))
        def _():
            s_copy(item, 1).wait_recv()
            pl.when(role(item, 1) & upward(item))(lambda: s_copy(item, 1).start())
            pl.when(role(item, 3) & jnp.logical_not(upward(item)))(lambda: s_copy(item, 3).start())
            c_copy(item).start()

    def far(item):
        @pl.when(role(item, 2))
        def _():
            s_copy(item, 1).wait_recv()
            c_copy(item).start()

    def across(g):
        took(l_all.at[pl.ds(0, g + 1), pl.ds(0, group)], c_recv.at[g])

    def each(act, g):
        for item in ITEMS:
            if item[0] == g:
                act(item)

    pl.when(core == 1)(lambda: pl.semaphore_wait(ack_core, 1))
    for k in range(1, RING):
        pl.when(k > x)(lambda k=k: pl.semaphore_wait(ack_x.at[k], 1))
    def x_copy(h, g, dy):
        return pltpu.make_async_remote_copy(src_ref=x_all.at[there(g, dy), :, within(h)], dst_ref=o_ref.at[:, cols(row, h)], send_sem=b_send,
                                            recv_sem=x_recv, device_id=(0, there(g, dy), col), device_id_type=MESH)

    def finish(h, g):
        from_line(g, b_all.at[pl.ds(0, RING), :, within(h)], b_all.at[pl.ds(0, RING - 1), :, within(h)], b_recv.at[h, g])
        depth, (start, width) = (g + 1) * group, PARTS[h]
        left = jnp.concatenate([l_all[k, g * group:(g + 1) * group, :] for k in range(2 * (g + 1))], axis=1)
        right = b_all[:(g + 1) * RING, :, start:start + width].reshape(depth, width)
        total = jnp.dot(left, right, preferred_element_type=jnp.float32)
        x_all[g * RING:(g + 1) * RING, :, start:start + width] = total.astype(jnp.bfloat16).reshape(RING, rows, width)
        others(g, lambda dy: x_copy(h, g, dy).start(), X_SHIFTS)

    stages = {'first': first, 'near': near, 'far': far}
    for name, *at in SEQUENCE:
        if name == 'across':
            across(*at)
        elif name == 'finish':
            finish(*at)
        else:
            each(stages[name], *at)
    o_ref[:, whole(row)] = x_all[row]

    units = pl.ds(0, group)
    for item in ITEMS:
        pl.when((z == item[0]) & role(item, 0))(lambda: took(l_all.at[0, pl.ds(0, 15 * rows)], l_send))
    for c in (0, 1):
        for v in range(RING):
            count = sent_along_x(c, v)
            assert 1 <= count <= 8
            pl.when((core == c) & (x == v))(lambda count=count: took(l_all.at[pl.ds(0, count), units], s_send))
    took(l_all.at[pl.ds(0, 5), pl.ds(0, 2 * group)], c_send)
    took(l_all.at[:, pl.ds(0, 15 * rows)], b_send)
    took(b_all.at[pl.ds(0, 15)], x_recv)


def sent_along_x(c, v):
    count = 0
    for (_, source), up in ITEMS.items():
        count += 2 if source == v else 0
        count += 1 if (v - source) % RING == (1 if up[c] else 3) else 0
    return count


def solution(mesh):
    block_spec = P(('batch', 'row'), 'col')
    dma, vmem, plain = pltpu.SemaphoreType.DMA, pltpu.VMEM, pltpu.SemaphoreType.REGULAR

    def step(l_block, b_block):
        rows, columns = b_block.shape
        return pl.pallas_call(
            kernel,
            out_shape=pltpu.VMEM(b_block.shape, b_block.dtype),
            in_specs=[pl.BlockSpec(memory_space=pl.ANY)] * 2,
            out_specs=pl.BlockSpec(memory_space=pltpu.VMEM),
            scratch_shapes=[
                vmem((rows, columns), jnp.bfloat16),
                vmem((16, rows, columns // 16), jnp.bfloat16),
                vmem((8, 16 * rows, 128), jnp.bfloat16),
                vmem((16, rows, columns // 16), jnp.bfloat16),
                dma((3,)), dma(()), dma((len(PARTS), RING)), dma(()), dma(()), dma((RING,)),
                dma(()), dma((len(ITEMS),)), dma(()), dma((RING,)), plain((RING,)), plain((RING,)), plain(()),
            ],
            compiler_params=pltpu.CompilerParams(collective_id=0, has_side_effects=True),
        )(l_block, b_block)

    return jax.shard_map(step, mesh=mesh, in_specs=(block_spec, block_spec), out_specs=block_spec, check_vma=False)
```

```python
import jax
import jax.numpy as jnp
from jax import lax
from jax.experimental import pallas as pl
from jax.experimental.pallas import tpu as pltpu
from jax.sharding import PartitionSpec as P

MESH = pl.DeviceIdType.MESH
RING = 4
PARTS = ((0, 256), (256, 256))
SEQUENCE = (
    ('first', 0),
    ('first', 1),
    ('first', 2),
    ('near', 0),
    ('first', 3),
    ('near', 1),
    ('far', 0),
    ('near', 2),
    ('across', 0),
    ('finish', 0, 0),
    ('far', 1),
    ('near', 3),
    ('across', 1),
    ('finish', 0, 1),
    ('far', 2),
    ('across', 2),
    ('finish', 0, 2),
    ('finish', 1, 0),
    ('far', 3),
    ('across', 3),
    ('finish', 0, 3),
    ('finish', 1, 1),
    ('finish', 1, 2),
    ('finish', 1, 3),
)
B_FIRST = ((0, 0), (1, 0))
B_ORDER = ((0, 1), (0, 2), (0, 3), (1, 1), (1, 2), (1, 3))
B_SHIFTS = (1, 3, 2, 0)
X_SHIFTS = (2, 1, 3, 0)
L_SHIFTS = (1, 3, 2, 0)
ITEMS = {
    (0, 0): (0, 0),
    (1, 0): (1, 1),
    (2, 0): (0, 0),
    (3, 0): (0, 0),
    (1, 1): (1, 1),
    (2, 1): (1, 1),
    (3, 1): (1, 1),
    (2, 2): (1, 1),
    (3, 2): (1, 1),
    (3, 3): (0, 0),
}


def kernel(l_ref, b_ref, o_ref, b_own, b_all, l_all, x_all, load_sem, b_send, b_recv, x_recv, l_send, l_recv, s_send,
           s_recv, c_send, c_recv, ack, ack_x, ack_core):
    row, col = lax.axis_index('row'), lax.axis_index('col')
    z, y, x, core = row // RING, row % RING, col // 2, col % 2
    rows, chunk = b_all.shape[1], b_all.shape[2]
    group = RING * rows
    partner = x * 2 + 1 - core

    def cols(r, h):
        return pl.ds(pl.multiple_of(r * chunk + PARTS[h][0], 128), PARTS[h][1])

    def within(h):
        return pl.ds(*PARTS[h])

    def whole(r):
        return pl.ds(pl.multiple_of(r * chunk, chunk), chunk)

    def there(g, dy):
        return g * RING + lax.rem(y + dy, RING)

    def others(g, act, shifts):
        for dy in shifts:
            if dy:
                act(dy)
            else:
                pl.when(z != g)(lambda: act(0))

    def piece(block):
        return l_all.at[block, pl.ds(pl.multiple_of(row * rows, rows), rows)]

    loads = [pltpu.make_async_copy(l_ref, piece(col), load_sem.at[0]), pltpu.make_async_copy(b_ref, b_own, load_sem.at[1]),
             pltpu.make_async_copy(b_ref.at[:, whole(row)], b_all.at[row], load_sem.at[2])]
    for copy in loads:
        copy.start()

    barrier = pltpu.get_barrier_semaphore()

    def greet(sem, to_row, to_col):
        pl.semaphore_signal(sem, inc=1, device_id=(0, to_row, to_col), device_id_type=MESH)

    pl.when(core == 1)(lambda: greet(barrier, row, partner))
    for r in range(1, RING * RING):
        pl.when(r > row)(lambda r=r: greet(barrier, r, col))
    for k in range(1, RING):
        pl.when(k > x)(lambda k=k: greet(barrier, row, k * 2 + core))
    pl.when(row + x + 1 - core > 0)(lambda: pl.semaphore_wait(barrier, row + x + 1 - core))
    for r in range(RING * RING - 1):
        pl.when(r < row)(lambda r=r: greet(ack.at[z], r, col))
    for k in range(RING - 1):
        pl.when(k < x)(lambda k=k: greet(ack_x.at[x - 1], row, k * 2 + core))
    pl.when(core == 0)(lambda: greet(ack_core, row, partner))
    loads[0].wait()

    def took(ref, sem):
        pltpu.make_async_copy(ref, ref, sem).wait()

    def from_line(g, four, three, sem):
        pl.when(z != g)(lambda: took(four, sem))
        pl.when(z == g)(lambda: took(three, sem))

    def block(item):
        return item[1] * 2 + core

    def role(item, shift):
        return lax.rem(x + RING - item[1], RING) == shift

    def to_x(k):
        return lax.rem(x + k, RING) * 2 + core

    def l_copy(item, g, dy):
        return pltpu.make_async_remote_copy(src_ref=piece(block(item)), dst_ref=piece(block(item)), send_sem=l_send, recv_sem=l_recv.at[item[0]],
                                            device_id=(0, there(g, dy), col), device_id_type=MESH)

    def spread(g):
        for item in ITEMS:
            pl.when((z == item[0]) & role(item, 0))(lambda item=item: others(g, lambda dy: l_copy(item, g, dy).start(), L_SHIFTS))

    def b_copy(h, g, dy):
        return pltpu.make_async_remote_copy(src_ref=b_own.at[:, cols(there(g, dy), h)], dst_ref=b_all.at[row, :, within(h)], send_sem=b_send,
                                            recv_sem=b_recv.at[h, z], device_id=(0, there(g, dy), col), device_id_type=MESH)

    def b_line(h, k):
        for dy in B_SHIFTS:
            if k or dy:
                b_copy(h, lax.rem(z + k, RING), dy).start()

    for g in range(RING):
        pl.when(g < z)(lambda g=g: spread(g))
    for g in range(RING):
        @pl.when(g == z)
        def _(g=g):
            pl.when(y < RING - 1)(lambda: pl.semaphore_wait(ack.at[g], RING - 1 - y))
            spread(g)
    loads[1].wait()
    for h, k in B_FIRST:
        b_line(h, k)
    for g in range(RING):
        @pl.when(g > z)
        def _(g=g):
            pl.semaphore_wait(ack.at[g], RING)
            spread(g)
    for h, k in B_ORDER:
        b_line(h, k)
    loads[2].wait()

    def s_copy(item, k):
        part = l_all.at[block(item), pl.ds(item[0] * group, group)]
        return pltpu.make_async_remote_copy(src_ref=part, dst_ref=part, send_sem=s_send, recv_sem=s_recv.at[list(ITEMS).index(item)],
                                            device_id=(0, row, to_x(k)), device_id_type=MESH)

    def c_copy(item):
        part = l_all.at[block(item), pl.ds(item[0] * group, group)]
        return pltpu.make_async_remote_copy(src_ref=part, dst_ref=part, send_sem=c_send, recv_sem=c_recv.at[item[0]],
                                            device_id=(0, row, partner), device_id_type=MESH)

    def upward(item):
        return jnp.where(core == 0, ITEMS[item][0], ITEMS[item][1]) == 1

    def first(item):
        @pl.when(role(item, 0))
        def _():
            from_line(item[0], l_all.at[0, pl.ds(0, group)], l_all.at[0, pl.ds(0, group - rows)], l_recv.at[item[0]])
            s_copy(item, 1).start()
            s_copy(item, 3).start()
            c_copy(item).start()

    def near(item):
        @pl.when(role(item, 1) | role(item, 3))
        def _():
            s_copy(item, 1).wait_recv()
            pl.when(role(item, 1) & upward(item))(lambda: s_copy(item, 1).start())
            pl.when(role(item, 3) & jnp.logical_not(upward(item)))(lambda: s_copy(item, 3).start())
            c_copy(item).start()

    def far(item):
        @pl.when(role(item, 2))
        def _():
            s_copy(item, 1).wait_recv()
            c_copy(item).start()

    def across(g):
        took(l_all.at[pl.ds(0, g + 1), pl.ds(0, group)], c_recv.at[g])

    def each(act, g):
        for item in ITEMS:
            if item[0] == g:
                act(item)

    pl.when(core == 1)(lambda: pl.semaphore_wait(ack_core, 1))
    for k in range(1, RING):
        pl.when(k > x)(lambda k=k: pl.semaphore_wait(ack_x.at[k - 1], 1))
    def x_copy(h, g, dy):
        return pltpu.make_async_remote_copy(src_ref=x_all.at[there(g, dy), :, within(h)], dst_ref=o_ref.at[:, cols(row, h)], send_sem=b_send,
                                            recv_sem=x_recv, device_id=(0, there(g, dy), col), device_id_type=MESH)

    def finish(h, g):
        from_line(g, b_all.at[pl.ds(0, RING), :, within(h)], b_all.at[pl.ds(0, RING - 1), :, within(h)], b_recv.at[h, g])
        depth, (start, width) = (g + 1) * group, PARTS[h]
        left = jnp.concatenate([l_all[k, g * group:(g + 1) * group, :] for k in range(2 * (g + 1))], axis=1)
        right = b_all[:(g + 1) * RING, :, start:start + width].reshape(depth, width)
        total = jnp.dot(left, right, preferred_element_type=jnp.float32)
        x_all[g * RING:(g + 1) * RING, :, start:start + width] = total.astype(jnp.bfloat16).reshape(RING, rows, width)
        others(g, lambda dy: x_copy(h, g, dy).start(), X_SHIFTS)

    stages = {'first': first, 'near': near, 'far': far}
    for name, *at in SEQUENCE:
        if name == 'across':
            across(*at)
        elif name == 'finish':
            finish(*at)
        else:
            each(stages[name], *at)
    o_ref[:, whole(row)] = x_all[row]

    units = pl.ds(0, group)
    for item in ITEMS:
        pl.when((z == item[0]) & role(item, 0))(lambda: took(l_all.at[0, pl.ds(0, 15 * rows)], l_send))
    for c in (0, 1):
        for v in range(RING):
            count = sent_along_x(c, v)
            assert 1 <= count <= 8
            pl.when((core == c) & (x == v))(lambda count=count: took(l_all.at[pl.ds(0, count), units], s_send))
    took(l_all.at[pl.ds(0, 5), pl.ds(0, 2 * group)], c_send)
    took(l_all.at[:, pl.ds(0, 15 * rows)], b_send)
    took(b_all.at[pl.ds(0, 15)], x_recv)


def sent_along_x(c, v):
    count = 0
    for (_, source), up in ITEMS.items():
        count += 2 if source == v else 0
        count += 1 if (v - source) % RING == (1 if up[c] else 3) else 0
    return count


def solution(mesh):
    block_spec = P(('batch', 'row'), 'col')
    dma, vmem, plain = pltpu.SemaphoreType.DMA, pltpu.VMEM, pltpu.SemaphoreType.REGULAR

    def step(l_block, b_block):
        rows, columns = b_block.shape
        return pl.pallas_call(
            kernel,
            out_shape=pltpu.VMEM(b_block.shape, b_block.dtype),
            in_specs=[pl.BlockSpec(memory_space=pl.ANY)] * 2,
            out_specs=pl.BlockSpec(memory_space=pltpu.VMEM),
            scratch_shapes=[
                vmem((rows, columns), jnp.bfloat16),
                vmem((16, rows, columns // 16), jnp.bfloat16),
                vmem((8, 16 * rows, 128), jnp.bfloat16),
                vmem((16, rows, columns // 16), jnp.bfloat16),
                dma((3,)), dma(()), dma((len(PARTS), RING)), dma(()), dma(()), dma((RING,)),
                dma(()), dma((len(ITEMS),)), dma(()), dma((RING,)), plain((RING,)), plain((RING - 1,)), plain(()),
            ],
            compiler_params=pltpu.CompilerParams(collective_id=0, has_side_effects=True),
        )(l_block, b_block)

    return jax.shard_map(step, mesh=mesh, in_specs=(block_spec, block_spec), out_specs=block_spec, check_vma=False)
```
